32 devices in a mesh: rep: 4 (over x, y), dp: 8 (over z, core).
Axes of the slice: x: 2, y: 2, z: 4, core: 2. Of those that a mesh axis runs over, the one named last changes fastest.
Arguments:
- x: bfloat16 [32, 4096, 512], P(('rep', 'dp')), parts along dimension 0
- dy: bfloat16 [32, 4096, 512], P(('rep', 'dp')), parts along dimension 0
- w_gate: bfloat16 [2, 512, 1664], P(None, 'dp')
- w_up: bfloat16 [2, 512, 1664], P(None, 'dp')
- w_down: bfloat16 [2, 1664, 512], P(None, 'dp')
- m_w_gate: float32 [2, 512, 1664], P(None, 'dp')
- m_w_up: float32 [2, 512, 1664], P(None, 'dp')
- m_w_down: float32 [2, 1664, 512], P(None, 'dp')
- v_w_gate: float32 [2, 512, 1664], P(None, 'dp')
- v_w_up: float32 [2, 512, 1664], P(None, 'dp')
- v_w_down: float32 [2, 1664, 512], P(None, 'dp')
Outputs:
- output 1: bfloat16 [8, 512, 1664], P('rep', 'dp'), parts along dimension 0
- output 2: bfloat16 [8, 512, 1664], P('rep', 'dp'), parts along dimension 0
- output 3: bfloat16 [8, 1664, 512], P('rep', 'dp'), parts along dimension 0
- output 4: float32 [8, 512, 1664], P('rep', 'dp'), parts along dimension 0
- output 5: float32 [8, 512, 1664], P('rep', 'dp'), parts along dimension 0
- output 6: float32 [8, 1664, 512], P('rep', 'dp'), parts along dimension 0
- output 7: float32 [8, 512, 1664], P('rep', 'dp'), parts along dimension 0
- output 8: float32 [8, 512, 1664], P('rep', 'dp'), parts along dimension 0
- output 9: float32 [8, 1664, 512], P('rep', 'dp'), parts along dimension 0
There are 4 independent parts. The reference program is written for one: setup_inputs(seed, part) draws one part's arguments, and reference() takes and returns one part's arrays. A program takes and returns all parts, laid end to end along the dimension named above; an argument that names none is the same for every part.
All inputs are finite; a program needn't handle non-finite values.
Results may differ from the reference program's by a relative error of at most 0.02.
Values are sent between devices in bfloat16 or wider.
A program may use at most 2 GiB of HBM per device.

```python
import jax
import jax.numpy as jnp
from jax import lax

SEQUENCES = 8
TOKENS = 4096
D = 512
FF = 1664
LAYERS = 2
NAMES = ("w_gate", "w_up", "w_down")
SHAPES = {"w_gate": (LAYERS, D, FF), "w_up": (LAYERS, D, FF), "w_down": (LAYERS, FF, D)}


def bump(key, n, height):
    away = (jnp.arange(n, dtype=jnp.int32) - jax.random.randint(key, (), 0, n, jnp.int32)) % n
    return jnp.where(away < n // 8, height, 1.0)


def together(key, own, strength):
    shared = jax.random.normal(key, own.shape[1:], jnp.float32)
    return (own + strength * shared) * lax.rsqrt(1 + strength * strength)


def setup_inputs(seed: int = 0, part: int = 0) -> dict:
    kx, kdy, ka, kb, kz, kf, kh, kl, *keys = jax.random.split(jax.random.key(seed), 8 + 3 * len(NAMES))
    kx, kdy, ka, kb = (jax.random.fold_in(k, part) for k in (kx, kdy, ka, kb))
    kw, km, kv = (keys[i::3] for i in range(3))
    shape = (SEQUENCES, TOKENS, D)
    much_x, much_dy = jax.random.uniform(kz, (2,), jnp.float32, 0.0, 1.0)
    loud = 2.0 ** jax.random.uniform(jax.random.fold_in(kz, 1), (), jnp.float32, -1.0, 2.0)
    layers = 2.0 ** jax.random.uniform(kl, (LAYERS, 1, 1), jnp.float32, -1.0, 1.0)
    x = together(ka, jax.random.normal(kx, shape, jnp.float32), much_x) * bump(kf, D, 4.0)
    dy = together(kb, jax.random.normal(kdy, shape, jnp.float32), much_dy)
    drawn = {"x": x.astype(jnp.bfloat16), "dy": (loud * dy * (SEQUENCES * TOKENS) ** -0.5).astype(jnp.bfloat16)}
    for key, name in zip(kw, NAMES, strict=True):
        w = jax.random.normal(key, SHAPES[name], jnp.float32) * SHAPES[name][1] ** -0.5
        drawn[name] = (w * {"w_gate": 1.0, "w_up": bump(kh, FF, 4.0), "w_down": layers}[name]).astype(jnp.bfloat16)
    for key, name in zip(km, NAMES, strict=True):
        drawn[f"m_{name}"] = 0.1 * jax.random.normal(key, SHAPES[name], jnp.float32)
    for key, name in zip(kv, NAMES, strict=True):
        drawn[f"v_{name}"] = jax.random.uniform(key, SHAPES[name], jnp.float32, 0.005, 0.015)
    return drawn


def matmul(a, w):
    return jnp.dot(a, w, preferred_element_type=jnp.float32).astype(jnp.bfloat16)


def normed(h):
    wide = h.astype(jnp.float32)
    scale = lax.rsqrt(jnp.mean(wide**2, -1, keepdims=True) + 1e-6)
    return (wide * scale).astype(jnp.bfloat16)


def layer(h, w):
    a = normed(h)
    gate = jnp.dot(a, w["w_gate"], preferred_element_type=jnp.float32)
    up = jnp.dot(a, w["w_up"], preferred_element_type=jnp.float32)
    return h + matmul((jax.nn.silu(gate) * up).astype(jnp.bfloat16), w["w_down"])


def adamw(w, m, v, g):
    m = 0.9 * m + 0.1 * g
    v = 0.95 * v + 0.05 * g * g
    step = m * lax.rsqrt(v + 1e-8) + 0.1 * w
    return (w - 0.02 * step).astype(jnp.bfloat16), m, v


def stack(weights, h):
    return lax.scan(lambda h, w: (layer(h, w), None), h, weights)[0]


def reference(x, dy, w_gate, w_up, w_down, m_w_gate, m_w_up, m_w_down, v_w_gate, v_w_up, v_w_down):
    weights = dict(zip(NAMES, (w_gate, w_up, w_down), strict=True))

    def take(so_far, sequence):
        h, by_y = sequence
        _, back = jax.vjp(lambda w: stack(w, h), weights)
        return jax.tree.map(lambda total, term: total + term.astype(jnp.float32), so_far, back(by_y)[0]), None

    none_yet = {name: jnp.zeros(w.shape, jnp.float32) for name, w in weights.items()}
    by_weights, _ = lax.scan(take, none_yet, (x, dy))
    gradients = [by_weights[name].astype(jnp.bfloat16).astype(jnp.float32) for name in NAMES]
    new = [
        adamw(w.astype(jnp.float32), m, v, g)
        for w, m, v, g in zip((w_gate, w_up, w_down), (m_w_gate, m_w_up, m_w_down), (v_w_gate, v_w_up, v_w_down), gradients, strict=True)
    ]
    return tuple(one[which] for which in range(3) for one in new)
```

```python
import functools

import jax
import jax.numpy as jnp
from jax import lax
from jax.experimental import pallas as pl
from jax.experimental.pallas import tpu as pltpu
from jax.sharding import PartitionSpec as P

T, D, FF = 4096, 512, 1664
UNITS = 13
GROUPS = 7
TILE = 512
TILES = T // TILE
VMEM_LIMIT = 67_043_328
BF, F32 = jnp.bfloat16, jnp.float32
BLOCKS = (UNITS, 2, 2, 2, 96, 256)


def dot(a, b):
    return lax.dot_general(a, b, (((1,), (0,)), ((), ())), preferred_element_type=F32)


def dot_nt(a, b):
    return lax.dot_general(a, b, (((1,), (1,)), ((), ())), preferred_element_type=F32)


def rms(h):
    wide = h.astype(F32)
    return wide, lax.rsqrt(jnp.mean(wide * wide, -1, keepdims=True) + 1e-6)


def place():
    me = lax.axis_index("dp")
    z1, z0, c = lax.div(me, 4), lax.rem(lax.div(me, 2), 2), lax.rem(me, 2)
    return z1, z0, c, (me + 1 - 2 * c, me + 2 - 4 * z0, me + 4 - 8 * z1)


def greet(partners):
    barrier = pltpu.get_barrier_semaphore()
    for p in partners:
        pl.semaphore_signal(barrier, inc=1, device_id={"dp": p}, device_id_type=pl.DeviceIdType.MESH)
    pl.semaphore_wait(barrier, 3)


def gather_copy(stage, u, w, send, recv, at):
    z1, z0, c, partners = at
    ref = (w.at[u, z1, z0, c], w.at[u, :, z0, c], w.at[u, :, :, c])[stage]
    return pltpu.make_async_remote_copy(
        src_ref=ref,
        dst_ref=ref,
        send_sem=send.at[stage, u],
        recv_sem=recv.at[stage, u],
        device_id={"dp": partners[2 - stage]},
        device_id_type=pl.DeviceIdType.MESH,
    )


def gather_tick(i, w, send, recv, at):
    @pl.when(i < UNITS)
    def _():
        gather_copy(0, i, w, send, recv, at).start()

    @pl.when((i >= 2) & (i < UNITS + 2))
    def _():
        gather_copy(0, i - 2, w, send, recv, at).wait_recv()
        gather_copy(1, i - 2, w, send, recv, at).start()

    @pl.when((i >= 4) & (i < UNITS + 4))
    def _():
        gather_copy(1, i - 4, w, send, recv, at).wait_recv()
        gather_copy(2, i - 4, w, send, recv, at).start()


def gather_ready(u, w, send, recv, at):
    gather_copy(2, u, w, send, recv, at).wait_recv()


def gather_end(w, send, recv, at):
    def one(u, carry):
        for stage in range(3):
            gather_copy(stage, u, w, send, recv, at).wait_send()
        return carry

    lax.fori_loop(0, UNITS, one, 0)


def scatter_copy(stage, s, n, bufs, send, recv, at):
    z1, z0, c, partners = at
    own, r1, r2, r3 = bufs
    u = pl.ds(2 * s, n)
    src = (own.at[u, :, :, 1 - c], r1.at[u, :, 1 - z0], r2.at[u, 1 - z1])[stage]
    dst = (r1, r2, r3)[stage].at[u]
    return pltpu.make_async_remote_copy(
        src_ref=src,
        dst_ref=dst,
        send_sem=send.at[stage, s],
        recv_sem=recv.at[stage, s],
        device_id={"dp": partners[stage]},
        device_id_type=pl.DeviceIdType.MESH,
    )


def scatter_advance(stage, s, n, bufs, g_ref, send, recv, at):
    z1, z0, c, partners = at
    own, r1, r2, r3 = bufs
    scatter_copy(stage, s, n, bufs, send, recv, at).wait_recv()
    for j in range(n):
        u = 2 * s + j
        if stage == 0:
            r1[u] = (r1[u].astype(F32) + own[u, :, :, c].astype(F32)).astype(BF)
        elif stage == 1:
            r2[u] = (r2[u].astype(F32) + r1[u, :, z0].astype(F32)).astype(BF)
        else:
            g_ref[u] = (r3[u].astype(F32) + r2[u, z1].astype(F32)).astype(BF)
    if stage < 2:
        scatter_copy(stage + 1, s, n, bufs, send, recv, at).start()


def scatter_end(bufs, send, recv, at):
    for stage in range(3):

        def one(s, carry, stage=stage):
            scatter_copy(stage, s, 2, bufs, send, recv, at).wait_send()
            return carry

        lax.fori_loop(0, GROUPS - 1, one, 0)
        scatter_copy(stage, GROUPS - 1, 1, bufs, send, recv, at).wait_send()


def tile_rows(t):
    return pl.ds(pl.multiple_of(t * TILE, TILE), TILE)


def forward_kernel(x_ref, own_ref, h_ref, w_out, a_ref, act_ref, w, send, recv, sem):
    at = place()
    z1, z0, c, partners = at
    bring = pltpu.make_async_copy(own_ref, w.at[:, z1, z0, c], sem.at[0])
    bring.start()
    greet(partners)
    bring.wait()
    for i in range(3):
        gather_tick(i, w, send, recv, at)

    def norm(t, carry):
        rows = tile_rows(t)
        wide, scale = rms(x_ref[rows, :])
        a_ref[rows, :] = (wide * scale).astype(BF)
        return carry

    lax.fori_loop(0, TILES, norm, 0)
    for i in range(3, 5):
        gather_tick(i, w, send, recv, at)

    def unit(u, carry):
        gather_tick(u + 5, w, send, recv, at)
        gather_ready(u, w, send, recv, at)
        columns = pl.ds(pl.multiple_of(u * 128, 128), 128)
        w_gu = w[u, :, :, :, :64, :].reshape(D, 256)

        def tile(t, carry):
            rows = tile_rows(t)
            gu = dot(a_ref[rows, :], w_gu)
            act_ref[rows, columns] = (jax.nn.silu(gu[:, :128]) * gu[:, 128:]).astype(BF)
            return carry

        return lax.fori_loop(0, TILES, tile, carry)

    lax.fori_loop(0, UNITS, unit, 0)
    save = pltpu.make_async_copy(w, w_out, sem.at[1])
    save.start()

    def down(t, carry):
        rows = tile_rows(t)
        act = act_ref[rows, :]
        for half in range(2):
            w_d = w[:, :, :, :, 64 + 16 * half : 80 + 16 * half, :].reshape(FF, 256)
            columns = slice(256 * half, 256 * half + 256)
            h_ref[rows, columns] = x_ref[rows, columns] + dot(act, w_d).astype(BF)
        return carry

    lax.fori_loop(0, TILES, down, 0)
    gather_end(w, send, recv, at)
    save.wait()


def backward_group(s, n, first, refs):
    a_ref, a_t, dy_ref, dy_t, da_ref, w, dgu_ref, act_ref, own = refs

    def tile(t, carry):
        rows = tile_rows(t)
        a, dy = a_ref[rows, :], dy_ref[rows, :]
        w_d = [w[pl.ds(2 * s, n), :, :, :, 64 + 16 * h : 80 + 16 * h, :].reshape(n * 128, 256) for h in range(2)]
        dact = dot_nt(dy[:, :256], w_d[0]) + dot_nt(dy[:, 256:], w_d[1])
        dact = dact.astype(BF).astype(F32)
        da = None
        for j in range(n):
            w_gu = w[2 * s + j, :, :, :, :64, :].reshape(D, 256)
            gu = dot(a, w_gu)
            gate, up = gu[:, :128], gu[:, 128:]
            sig = jax.nn.sigmoid(gate)
            silu = gate * sig
            act_ref[rows, 128 * j : 128 * j + 128] = (silu * up).astype(BF)
            mine = dact[:, 128 * j : 128 * j + 128]
            dgate = mine * up * (sig + silu * (1 - sig))
            dgu = jnp.concatenate([dgate.astype(BF), (mine * silu).astype(BF)], axis=1)
            dgu_ref[j, rows, :] = dgu
            if not first:
                term = dot_nt(dgu, w_gu)
                da = term if da is None else da + term
        if not first:
            da_ref[rows, :] += da
        return carry

    lax.fori_loop(0, TILES, tile, 0)
    for j in range(n):
        by_gu = dot(a_t[...], dgu_ref[j]).astype(BF)
        own[2 * s + j, :, :, :, :64, :] = by_gu.reshape(2, 2, 2, 64, 256)
    by_d = dot(dy_t[...], act_ref[:, : 128 * n])
    for j in range(n):
        for h in range(2):
            piece = by_d[256 * h : 256 * h + 256, 128 * j : 128 * j + 128].T.astype(BF)
            own[2 * s + j, :, :, :, 64 + 16 * h : 80 + 16 * h, :] = piece.reshape(2, 2, 2, 16, 256)


def backward_all(first, refs, bufs, g_ref, send, recv, at, before):
    def advance(s):
        for stage in range(3):

            @pl.when(s >= stage + 1)
            def _(stage=stage):
                scatter_advance(stage, s - 1 - stage, 2, bufs, g_ref, send, recv, at)

    def group(s, carry):
        before(s, 2)
        backward_group(s, 2, first, refs)
        advance(s)
        scatter_copy(0, s, 2, bufs, send, recv, at).start()
        return carry

    last = GROUPS - 1
    lax.fori_loop(0, last, group, 0)
    before(last, 1)
    backward_group(last, 1, first, refs)
    for stage in range(3):
        scatter_advance(stage, last - 1 - stage, 2, bufs, g_ref, send, recv, at)
    scatter_copy(0, last, 1, bufs, send, recv, at).start()


def backward_drain(bufs, g_ref, send, recv, at):
    last = GROUPS - 1
    scatter_advance(0, last, 1, bufs, g_ref, send, recv, at)
    scatter_advance(1, last - 1, 2, bufs, g_ref, send, recv, at)
    scatter_advance(2, last - 2, 2, bufs, g_ref, send, recv, at)
    scatter_advance(1, last, 1, bufs, g_ref, send, recv, at)
    scatter_advance(2, last - 1, 2, bufs, g_ref, send, recv, at)
    scatter_advance(2, last, 1, bufs, g_ref, send, recv, at)
    scatter_end(bufs, send, recv, at)


def set_out(h_ref, dy_ref, a_ref, a_t, dy_t, da_ref):
    def one(t, carry):
        rows = tile_rows(t)
        wide, scale = rms(h_ref[rows, :])
        a = (wide * scale).astype(BF)
        a_ref[rows, :] = a
        a_t[:, rows] = a.T
        dy_t[:, rows] = dy_ref[rows, :].T
        if da_ref is not None:
            da_ref[rows, :] = jnp.zeros((TILE, D), F32)
        return carry

    lax.fori_loop(0, TILES, one, 0)


def last_layer_kernel(
    h_ref, dy_ref, own_w, dh_ref, g_ref, a_ref, a_t, dy_t, da_ref, w, dgu_ref, act_ref, own, r1, r2, r3, wsend, wrecv, send, recv, sem
):
    at = place()
    z1, z0, c, partners = at
    bring = pltpu.make_async_copy(own_w, w.at[:, z1, z0, c], sem.at[0])
    bring.start()
    greet(partners)
    bring.wait()
    for i in range(3):
        gather_tick(i, w, wsend, wrecv, at)
    set_out(h_ref, dy_ref, a_ref, a_t, dy_t, da_ref)
    for i in range(3, 5):
        gather_tick(i, w, wsend, wrecv, at)

    def before(s, n):
        for j in range(n):
            gather_tick(2 * s + j + 5, w, wsend, wrecv, at)
        for j in range(n):
            gather_ready(2 * s + j, w, wsend, wrecv, at)

    bufs = (own, r1, r2, r3)
    backward_all(False, (a_ref, a_t, dy_ref, dy_t, da_ref, w, dgu_ref, act_ref, own), bufs, g_ref, send, recv, at, before)

    def norm(t, carry):
        rows = tile_rows(t)
        wide, scale = rms(h_ref[rows, :])
        da = da_ref[rows, :].astype(BF).astype(F32)
        along = jnp.sum(da * wide, -1, keepdims=True) * (scale * scale * scale * (1.0 / D))
        by_h = (da * scale - wide * along).astype(BF)
        dh_ref[rows, :] = dy_ref[rows, :] + by_h
        return carry

    lax.fori_loop(0, TILES, norm, 0)
    gather_end(w, wsend, wrecv, at)
    backward_drain(bufs, g_ref, send, recv, at)


def first_layer_kernel(h_ref, dy_ref, w, g_ref, a_ref, a_t, dy_t, dgu_ref, act_ref, own, r1, r2, r3, send, recv):
    at = place()
    greet(at[3])
    set_out(h_ref, dy_ref, a_ref, a_t, dy_t, None)
    bufs = (own, r1, r2, r3)
    refs = (a_ref, a_t, dy_ref, dy_t, None, w, dgu_ref, act_ref, own)
    backward_all(True, refs, bufs, g_ref, send, recv, at, lambda s, n: None)
    backward_drain(bufs, g_ref, send, recv, at)


def vmem(*shape):
    return pltpu.VMEM(shape, BF)


IN_VMEM = pl.BlockSpec(memory_space=pltpu.VMEM)
ANYWHERE = pl.BlockSpec(memory_space=pl.ANY)
DMA = pltpu.SemaphoreType.DMA


def call(kernel, name, number, in_specs, out, out_specs, scratch, flops):
    return pl.pallas_call(
        kernel,
        name=name,
        out_shape=out,
        in_specs=in_specs,
        out_specs=out_specs,
        scratch_shapes=scratch,
        compiler_params=pltpu.CompilerParams(collective_id=number, has_side_effects=True, vmem_limit_bytes=VMEM_LIMIT),
        cost_estimate=pl.CostEstimate(flops=flops, bytes_accessed=20_000_000, transcendentals=0),
    )


def shape(*dims):
    return jax.ShapeDtypeStruct(dims, BF)


MATMUL = 2 * T * D * FF
SUMS = [
    vmem(*BLOCKS),
    vmem(UNITS, 2, 2, 96, 256),
    vmem(UNITS, 2, 96, 256),
    vmem(UNITS, 96, 256),
]


def forward(x, own):
    return call(
        forward_kernel,
        "forward",
        0,
        [IN_VMEM, ANYWHERE],
        (shape(T, D), shape(*BLOCKS)),
        (IN_VMEM, ANYWHERE),
        [vmem(T, D), vmem(T, FF), vmem(*BLOCKS), DMA((3, UNITS)), DMA((3, UNITS)), DMA((2,))],
        3 * MATMUL,
    )(x, own)


def last_layer(h, dy, own):
    return call(
        last_layer_kernel,
        "last_layer",
        1,
        [IN_VMEM, IN_VMEM, ANYWHERE],
        (shape(T, D), shape(UNITS, 96, 256)),
        (IN_VMEM, IN_VMEM),
        [
            vmem(T, D),
            vmem(D, T),
            vmem(D, T),
            pltpu.VMEM((T, D), F32),
            vmem(*BLOCKS),
            vmem(2, T, 256),
            vmem(T, 256),
            *SUMS,
            DMA((3, UNITS)),
            DMA((3, UNITS)),
            DMA((3, GROUPS)),
            DMA((3, GROUPS)),
            DMA((1,)),
        ],
        8 * MATMUL,
    )(h, dy, own)


def first_layer(x, dh, w):
    return call(
        first_layer_kernel,
        "first_layer",
        2,
        [IN_VMEM, IN_VMEM, IN_VMEM],
        shape(UNITS, 96, 256),
        IN_VMEM,
        [vmem(T, D), vmem(D, T), vmem(D, T), vmem(2, T, 256), vmem(T, 256), *SUMS, DMA((3, GROUPS)), DMA((3, GROUPS))],
        6 * MATMUL,
    )(x, dh, w)


def to_units(w_gate, w_up, w_down):
    layers = w_gate.shape[0]
    wide = [w.reshape(layers, 64, 8, UNITS, 16).transpose(0, 3, 1, 2, 4).reshape(layers, UNITS, 64, 128) for w in (w_gate, w_up)]
    down = w_down.reshape(layers, UNITS, 16, 2, 256).transpose(0, 1, 3, 2, 4).reshape(layers, UNITS, 32, 256)
    return jnp.concatenate([jnp.concatenate(wide, -1), down], 2)


def from_units(g):
    layers = g.shape[0]
    wide = [
        g[:, :, :64, at : at + 128].reshape(layers, UNITS, 64, 8, 16).transpose(0, 2, 3, 1, 4).reshape(layers, 64, FF) for at in (0, 128)
    ]
    down = g[:, :, 64:].reshape(layers, UNITS, 2, 16, 256).transpose(0, 1, 3, 2, 4).reshape(layers, 208, D)
    return *wide, down


def adamw(w, m, v, g):
    m = 0.9 * m + 0.1 * g
    v = 0.95 * v + 0.05 * g * g
    step = m * lax.rsqrt(v + 1e-8) + 0.1 * w
    return (w - 0.02 * step).astype(BF), m, v


def solution(mesh):
    def step(x, dy, *arrays):
        weights, m, v = (arrays[i : i + 3] for i in (0, 3, 6))
        own = to_units(*weights)
        h, w0 = forward(x[0], own[0])
        dh, g1 = last_layer(h, dy[0], own[1])
        g0 = first_layer(x[0], dh, w0)
        gradients = from_units(jnp.stack([g0, g1]))
        new = [adamw(w.astype(F32), m, v, g.astype(F32)) for w, m, v, g in zip(weights, m, v, gradients, strict=True)]
        return tuple(one[which] for which in range(3) for one in new)

    states, cut = P(("rep", "dp"), None, None), P(None, "dp", None)
    return jax.shard_map(
        step,
        mesh=mesh,
        in_specs=(states, states) + (cut,) * 9,
        out_specs=(P("rep", "dp", None),) * 9,
        check_vma=False,
    )
```

```python
import functools

import jax
import jax.numpy as jnp
from jax import lax
from jax.experimental import pallas as pl
from jax.experimental.pallas import tpu as pltpu
from jax.sharding import PartitionSpec as P

T, D, FF = 4096, 512, 1664
UNITS = 13
GROUPS = 7
TILE = 512
VMEM_LIMIT = 67_043_328
BF, F32 = jnp.bfloat16, jnp.float32
BOTH = 2 * UNITS


def dot(a, b):
    return lax.dot_general(a, b, (((1,), (0,)), ((), ())), preferred_element_type=F32)


def dot_nt(a, b):
    return lax.dot_general(a, b, (((1,), (1,)), ((), ())), preferred_element_type=F32)


def rms(h):
    wide = h.astype(F32)
    return wide, lax.rsqrt(jnp.mean(wide * wide, -1, keepdims=True) + 1e-6)


def place():
    me = lax.axis_index("dp")
    z1, z0, c = lax.div(me, 4), lax.rem(lax.div(me, 2), 2), lax.rem(me, 2)
    return z1, z0, c, (me + 1 - 2 * c, me + 2 - 4 * z0, me + 4 - 8 * z1)


def greet(partners):
    barrier = pltpu.get_barrier_semaphore()
    for p in partners:
        pl.semaphore_signal(barrier, inc=1, device_id={"dp": p}, device_id_type=pl.DeviceIdType.MESH)
    pl.semaphore_wait(barrier, 3)


def gather_copy(stage, u, w, send, recv, at):
    z1, z0, c, partners = at
    ref = (w.at[u, z1, z0, c], w.at[u, :, z0, c], w.at[u, :, :, c])[stage]
    return pltpu.make_async_remote_copy(
        src_ref=ref,
        dst_ref=ref,
        send_sem=send.at[stage, u],
        recv_sem=recv.at[stage, u],
        device_id={"dp": partners[2 - stage]},
        device_id_type=pl.DeviceIdType.MESH,
    )


def gather_tick(i, w, send, recv, at):
    @pl.when(i < BOTH)
    def _():
        gather_copy(0, i, w, send, recv, at).start()

    @pl.when((i >= 2) & (i < BOTH + 2))
    def _():
        gather_copy(0, i - 2, w, send, recv, at).wait_recv()
        gather_copy(1, i - 2, w, send, recv, at).start()

    @pl.when((i >= 4) & (i < BOTH + 4))
    def _():
        gather_copy(1, i - 4, w, send, recv, at).wait_recv()
        gather_copy(2, i - 4, w, send, recv, at).start()


def gather_ready(u, w, send, recv, at):
    gather_copy(2, u, w, send, recv, at).wait_recv()


def gather_sent(u, w, send, recv, at):
    for stage in range(3):
        gather_copy(stage, u, w, send, recv, at).wait_send()


def scatter_copy(stage, u, n, bufs, send, recv, at):
    z1, z0, c, partners = at
    own, r1, r2, r3 = bufs
    us = pl.ds(u, n)
    src = (own.at[us, :, :, 1 - c], r1.at[us, :, 1 - z0], r2.at[us, 1 - z1])[stage]
    dst = (r1, r2, r3)[stage].at[us]
    return pltpu.make_async_remote_copy(
        src_ref=src,
        dst_ref=dst,
        send_sem=send.at[stage, u],
        recv_sem=recv.at[stage, u],
        device_id={"dp": partners[stage]},
        device_id_type=pl.DeviceIdType.MESH,
    )


def scatter_advance(stage, u, n, bufs, g_ref, send, recv, at):
    z1, z0, c, partners = at
    own, r1, r2, r3 = bufs
    scatter_copy(stage, u, n, bufs, send, recv, at).wait_recv()
    for v in range(n):
        v = u + v
        if stage == 0:
            r1[v] = (r1[v].astype(F32) + own[v, :, :, c].astype(F32)).astype(BF)
        elif stage == 1:
            r2[v] = (r2[v].astype(F32) + r1[v, :, z0].astype(F32)).astype(BF)
        else:
            g_ref[v] = (r3[v].astype(F32) + r2[v, z1].astype(F32)).astype(BF)
    if stage < 2:
        scatter_copy(stage + 1, u, n, bufs, send, recv, at).start()


def over(tile, body):
    def one(t, carry):
        body(pl.ds(pl.multiple_of(t * tile, tile), tile))
        return carry

    lax.fori_loop(0, T // tile, one, 0)


def groups(body):
    def one(s, carry):
        body(s, 2)
        return carry

    lax.fori_loop(0, GROUPS - 1, one, 0)
    body(GROUPS - 1, 1)


def w_gu_of(w, u):
    return w[u, :, :, :, :64, :].reshape(D, 256)


def w_d_of(w, u, n, half):
    return w[pl.ds(u, n), :, :, :, 64 + 16 * half : 80 + 16 * half, :].reshape(n * 128, 256)


def forward_group(u, n, a_ref, acc_ref, w):
    def tile(rows):
        a = a_ref[rows, :]
        act = []
        for j in range(n):
            gu = dot(a, w_gu_of(w, u + j))
            act.append((jax.nn.silu(gu[:, :128]) * gu[:, 128:]).astype(BF))
        act = jnp.concatenate(act, axis=1) if n > 1 else act[0]
        for half in range(2):
            columns = slice(256 * half, 256 * half + 256)
            acc_ref[rows, columns] += dot(act, w_d_of(w, u, n, half))

    over(TILE, tile)


def backward_group(u, n, first, refs, sent):
    a_ref, a_t, dy_ref, dy_t, da_ref, w, w_t, w_dt, dgu_ref, act_ref = refs
    for j in range(n):
        if not first:
            w_t[256 * j : 256 * j + 256, :] = w_gu_of(w, u + j).T
    for half in range(2):
        w_dt[256 * half : 256 * half + 256, : 128 * n] = w_d_of(w, u, n, half).T

    def tile(rows):
        a = a_ref[rows, :]
        dact = dot(dy_ref[rows, :], w_dt[:, : 128 * n]).astype(BF).astype(F32)
        for j in range(n):
            gu = dot(a, w_gu_of(w, u + j))
            gate, up = gu[:, :128], gu[:, 128:]
            sig = jax.nn.sigmoid(gate)
            silu = gate * sig
            mine = dact[:, 128 * j : 128 * j + 128]
            act_ref[rows, 128 * j : 128 * j + 128] = (silu * up).astype(BF)
            dgu_ref[rows, 256 * j : 256 * j + 128] = (mine * up * (sig + silu * (1 - sig))).astype(BF)
            dgu_ref[rows, 256 * j + 128 : 256 * j + 256] = (mine * silu).astype(BF)
        if not first:
            da_ref[rows, :] += dot(dgu_ref[rows, : 256 * n], w_t[: 256 * n, :])

    over(TILE, tile)
    for j in range(n):
        sent(u + j)
        by_gu = dot(a_t[...], dgu_ref[:, 256 * j : 256 * j + 256]).astype(BF)
        w[u + j, :, :, :, :64, :] = by_gu.reshape(2, 2, 2, 64, 256)
    by_d = dot(dy_t[...], act_ref[:, : 128 * n])
    for j in range(n):
        for h in range(2):
            piece = by_d[256 * h : 256 * h + 256, 128 * j : 128 * j + 128].T.astype(BF)
            w[u + j, :, :, :, 64 + 16 * h : 80 + 16 * h, :] = piece.reshape(2, 2, 2, 16, 256)


def normed(h):
    wide, scale = rms(h)
    return (wide * scale).astype(BF)


def kernel(
    x_ref, dy_in, own, g_ref, h_ref, a_ref, a_t, dy_ref, dy_t, acc_ref, w, w_t, w_dt, dgu_ref, act_ref, r1, r2, r3, gsend, grecv, ssend, srecv, sem
):
    at = place()
    z1, z0, c, partners = at
    halves = [pl.ds(0, UNITS), pl.ds(UNITS, UNITS)]
    bring = [pltpu.make_async_copy(own.at[us], w.at[us, z1, z0, c], sem.at[i]) for i, us in enumerate(halves)]
    bring += [pltpu.make_async_copy(x_ref, h_ref, sem.at[2]), pltpu.make_async_copy(dy_in, dy_ref, sem.at[3])]
    for copy in (bring[0], bring[2], bring[1], bring[3]):
        copy.start()
    greet(partners)
    gather = functools.partial(gather_tick, w=w, send=gsend, recv=grecv, at=at)
    bring[0].wait()
    for i in range(3):
        gather(i)
    bring[2].wait()

    def enter(rows):
        a_ref[rows, :] = normed(h_ref[rows, :])
        acc_ref[rows, :] = jnp.zeros((TILE, D), F32)

    over(TILE, enter)
    bring[1].wait()
    for i in range(3, 5):
        gather(i)

    def fetched(u, n):
        for j in range(n):
            gather(u + j + 5)
        for j in range(n):
            gather_ready(u + j, w, gsend, grecv, at)

    def forward(s, n):
        fetched(2 * s, n)
        forward_group(2 * s, n, a_ref, acc_ref, w)

    groups(forward)
    bring[3].wait()

    def between(rows):
        h = h_ref[rows, :] + acc_ref[rows, :].astype(BF)
        h_ref[rows, :] = h
        a = normed(h)
        a_ref[rows, :] = a
        a_t[:, rows] = a.T
        dy_t[:, rows] = dy_ref[rows, :].T
        acc_ref[rows, :] = jnp.zeros((TILE, D), F32)

    over(TILE, between)

    bufs = (w, r1, r2, r3)
    refs = (a_ref, a_t, dy_ref, dy_t, acc_ref, w, w_t, w_dt, dgu_ref, act_ref)

    def sent(u):
        gather_sent(u, w, gsend, grecv, at)

    def advance(stage, u, n):
        scatter_advance(stage, u, n, bufs, g_ref, ssend, srecv, at)

    def set_out(u, n):
        scatter_copy(0, u, n, bufs, ssend, srecv, at).start()

    end = UNITS - 1

    def layer1(s, n):
        u = UNITS + 2 * s
        fetched(u, n)
        backward_group(u, n, False, refs, sent)
        for stage in range(3):
            back = u - 2 - 2 * stage

            @pl.when(back >= UNITS)
            def _(stage=stage, back=back):
                advance(stage, back, 2)

        set_out(u, n)

    groups(layer1)
    again = pltpu.make_async_copy(x_ref, a_ref, sem.at[2])
    again.start()

    def leave(rows):
        wide, scale = rms(h_ref[rows, :])
        da = acc_ref[rows, :].astype(BF).astype(F32)
        along = jnp.sum(da * wide, -1, keepdims=True) * (scale * scale * scale * (1.0 / D))
        dh = dy_ref[rows, :] + (da * scale - wide * along).astype(BF)
        dy_ref[rows, :] = dh
        dy_t[:, rows] = dh.T

    over(TILE, leave)
    again.wait()

    def enter_again(rows):
        a = normed(a_ref[rows, :])
        a_ref[rows, :] = a
        a_t[:, rows] = a.T

    over(TILE, enter_again)

    def layer0(s, n):
        u = 2 * s
        backward_group(u, n, True, refs, sent)
        for stage in range(3):
            back = u - 2 - 2 * stage

            @pl.when(back >= 0)
            def _(stage=stage, back=back):
                advance(stage, back, 2)

            @pl.when(back == -2)
            def _(stage=stage):
                advance(stage, BOTH - 1, 1)

            if stage:

                @pl.when(back < -2)
                def _(stage=stage, back=back):
                    advance(stage, back + BOTH + 1, 2)

        set_out(u, n)

    groups(layer0)
    for stage, u, n in ((0, end, 1), (1, end - 2, 2), (2, end - 4, 2), (1, end, 1), (2, end - 2, 2), (2, end, 1)):
        advance(stage, u, n)
    for stage in range(3):
        for base in (UNITS, 0):

            def one(s, carry, stage=stage, base=base):
                scatter_copy(stage, base + 2 * s, 2, bufs, ssend, srecv, at).wait_send()
                return carry

            lax.fori_loop(0, GROUPS - 1, one, 0)
            scatter_copy(stage, base + end, 1, bufs, ssend, srecv, at).wait_send()


def vmem(*shape):
    return pltpu.VMEM(shape, BF)


IN_VMEM = pl.BlockSpec(memory_space=pltpu.VMEM)
ANYWHERE = pl.BlockSpec(memory_space=pl.ANY)
DMA = pltpu.SemaphoreType.DMA


def gradients_of(x, dy, own):
    return pl.pallas_call(
        kernel,
        name="both_layers",
        out_shape=jax.ShapeDtypeStruct((BOTH, 96, 256), BF),
        in_specs=[ANYWHERE] * 3,
        out_specs=IN_VMEM,
        scratch_shapes=[
            vmem(T, D),
            vmem(T, D),
            vmem(D, T),
            vmem(T, D),
            vmem(D, T),
            pltpu.VMEM((T, D), F32),
            vmem(BOTH, 2, 2, 2, 96, 256),
            vmem(512, D),
            vmem(D, 256),
            vmem(T, 512),
            vmem(T, 256),
            vmem(BOTH, 2, 2, 96, 256),
            vmem(BOTH, 2, 96, 256),
            vmem(BOTH, 96, 256),
            *[DMA((3, BOTH))] * 4,
            DMA((4,)),
        ],
        compiler_params=pltpu.CompilerParams(collective_id=0, has_side_effects=True, vmem_limit_bytes=VMEM_LIMIT),
        cost_estimate=pl.CostEstimate(flops=34 * T * D * FF, bytes_accessed=20_000_000, transcendentals=0),
    )(x, dy, own)


def to_units(w_gate, w_up, w_down):
    layers = w_gate.shape[0]
    wide = [w.reshape(layers, 64, 8, UNITS, 16).transpose(0, 3, 1, 2, 4).reshape(layers, UNITS, 64, 128) for w in (w_gate, w_up)]
    down = w_down.reshape(layers, UNITS, 16, 2, 256).transpose(0, 1, 3, 2, 4).reshape(layers, UNITS, 32, 256)
    return jnp.concatenate([jnp.concatenate(wide, -1), down], 2)


def from_units(g):
    layers = g.shape[0]
    wide = [
        g[:, :, :64, at : at + 128].reshape(layers, UNITS, 64, 8, 16).transpose(0, 2, 3, 1, 4).reshape(layers, 64, FF) for at in (0, 128)
    ]
    down = g[:, :, 64:].reshape(layers, UNITS, 2, 16, 256).transpose(0, 1, 3, 2, 4).reshape(layers, 208, D)
    return *wide, down


def adamw(w, m, v, g):
    m = 0.9 * m + 0.1 * g
    v = 0.95 * v + 0.05 * g * g
    step = m * lax.rsqrt(v + 1e-8) + 0.1 * w
    return (w - 0.02 * step).astype(BF), m, v


def solution(mesh):
    def step(x, dy, *arrays):
        weights, m, v = (arrays[i : i + 3] for i in (0, 3, 6))
        own = to_units(*weights)
        g = gradients_of(x[0], dy[0], own.reshape(BOTH, 96, 256))
        gradients = from_units(g.reshape(own.shape))
        new = [adamw(w.astype(F32), m, v, g.astype(F32)) for w, m, v, g in zip(weights, m, v, gradients, strict=True)]
        return tuple(one[which] for which in range(3) for one in new)

    states, cut = P(("rep", "dp"), None, None), P(None, "dp", None)
    return jax.shard_map(
        step,
        mesh=mesh,
        in_specs=(states, states) + (cut,) * 9,
        out_specs=(P("rep", "dp", None),) * 9,
        check_vma=False,
    )
```

```python
import functools

import jax
import jax.numpy as jnp
from jax import lax
from jax.experimental import pallas as pl
from jax.experimental.pallas import tpu as pltpu
from jax.sharding import PartitionSpec as P

T, D, FF = 4096, 512, 1664
UNITS = 13
GROUPS = 7
TILE = 1024
ROWS = 512
PAIRS = UNITS
VMEM_LIMIT = 67_043_328
BF, F32 = jnp.bfloat16, jnp.float32
BOTH = 2 * UNITS


def dot(a, b):
    return lax.dot_general(a, b, (((1,), (0,)), ((), ())), preferred_element_type=F32)


def dot_nt(a, b):
    return lax.dot_general(a, b, (((1,), (1,)), ((), ())), preferred_element_type=F32)


def rms(h):
    wide = h.astype(F32)
    return wide, lax.rsqrt(jnp.mean(wide * wide, -1, keepdims=True) + 1e-6)


def place():
    me, rep = lax.axis_index("dp"), lax.axis_index("rep")
    z1, z0, c = lax.div(me, 4), lax.rem(lax.div(me, 2), 2), lax.rem(me, 2)
    x, y = lax.div(rep, 2), lax.rem(rep, 2)
    return z1, z0, c, (me + 1 - 2 * c, me + 2 - 4 * z0, me + 4 - 8 * z1), (x, y), (rep + 2 - 4 * x, rep + 1 - 2 * y)


def greet(at):
    barrier = pltpu.get_barrier_semaphore()
    for axis, partners in (("dp", at[3]), ("rep", at[5])):
        for p in partners:
            pl.semaphore_signal(barrier, inc=1, device_id={axis: p}, device_id_type=pl.DeviceIdType.MESH)
    pl.semaphore_wait(barrier, 5)


def turn(i, of):
    return of[0] + lax.rem(i, 2) * (of[1] - of[0])


def mine_of(i, at):
    return 2 * i + turn(i, at[4])


def gather_copy(stage, u, w, send, recv, at):
    z1, z0, c, partners, _, sides = at
    ref = (w.at[u, z1, z0, c], w.at[u, :, z0, c], w.at[u, :, :, c], w.at[u, :, :, c])[stage]
    to = ({"dp": partners[2]}, {"dp": partners[1]}, {"rep": turn(lax.div(u, 2), sides)}, {"dp": partners[0]})[stage]
    return pltpu.make_async_remote_copy(
        src_ref=ref,
        dst_ref=ref,
        send_sem=send.at[stage, u],
        recv_sem=recv.at[stage, u],
        device_id=to,
        device_id_type=pl.DeviceIdType.MESH,
    )


def gather_tick(i, w, send, recv, at):
    def copy(stage, u):
        return gather_copy(stage, u, w, send, recv, at)

    @pl.when(i < PAIRS)
    def _():
        copy(0, mine_of(i, at)).start()

    @pl.when((i >= 2) & (i < PAIRS + 1))
    def _():
        u = mine_of(i - 1, at)
        copy(0, u).wait_recv()
        copy(1, u).start()

    @pl.when((i >= 3) & (i < PAIRS + 2))
    def _():
        u = mine_of(i - 2, at)
        copy(1, u).wait_recv()
        copy(2, u).start()
        copy(3, u).start()

    @pl.when((i >= 4) & (i < PAIRS + 3))
    def _():
        u = 4 * (i - 3) + 1 - mine_of(i - 3, at)
        copy(2, u).wait_recv()
        copy(3, u).start()


def gather_first(tick, w, send, recv, at):
    for stage in range(3):
        for u in range(2):
            if stage:
                gather_copy(stage - 1, u, w, send, recv, at).wait_recv()
            gather_copy(stage + stage // 2, u, w, send, recv, at).start()
        tick(stage + 1)


def gather_ready(u, w, send, recv, at):
    gather_copy(3, u, w, send, recv, at).wait_recv()


def gather_sent(u, w, send, recv, at):
    i = lax.div(u, 2)
    mine = u == mine_of(i, at)
    for stage, sent in ((0, mine | (i == 0)), (1, mine | (i == 0)), (2, mine & (i > 0))):

        @pl.when(sent)
        def _(stage=stage):
            gather_copy(stage, u, w, send, recv, at).wait_send()

    gather_copy(3, u, w, send, recv, at).wait_send()


def scatter_copy(stage, u, n, bufs, send, recv, at):
    z1, z0, c, partners = at[:4]
    own, r1, r2, r3 = bufs
    us = pl.ds(u, n)
    src = (own.at[us, :, :, 1 - c], r1.at[us, :, 1 - z0], r2.at[us, 1 - z1])[stage]
    dst = (r1, r2, r3)[stage].at[us]
    return pltpu.make_async_remote_copy(
        src_ref=src,
        dst_ref=dst,
        send_sem=send.at[stage, u],
        recv_sem=recv.at[stage, u],
        device_id={"dp": partners[stage]},
        device_id_type=pl.DeviceIdType.MESH,
    )


def scatter_advance(stage, u, n, bufs, g_ref, send, recv, at):
    z1, z0, c, partners = at[:4]
    own, r1, r2, r3 = bufs
    scatter_copy(stage, u, n, bufs, send, recv, at).wait_recv()
    for v in range(n):
        v = u + v
        if stage == 0:
            r1[v] = (r1[v].astype(F32) + own[v, :, :, c].astype(F32)).astype(BF)
        elif stage == 1:
            r2[v] = (r2[v].astype(F32) + r1[v, :, z0].astype(F32)).astype(BF)
        else:
            g_ref[v] = (r3[v].astype(F32) + r2[v, z1].astype(F32)).astype(BF)
    if stage < 2:
        scatter_copy(stage + 1, u, n, bufs, send, recv, at).start()


def over(tile, body):
    def one(t, carry):
        body(pl.ds(pl.multiple_of(t * tile, tile), tile))
        return carry

    lax.fori_loop(0, T // tile, one, 0)


def groups(body):
    def one(s, carry):
        body(s, 2)
        return carry

    lax.fori_loop(0, GROUPS - 1, one, 0)
    body(GROUPS - 1, 1)


def w_gu_of(w, u):
    return w[u, :, :, :, :64, :].reshape(D, 256)


def w_d_of(w, u, n, half):
    return w[pl.ds(u, n), :, :, :, 64 + 16 * half : 80 + 16 * half, :].reshape(n * 128, 256)


def forward_group(u, n, a_ref, acc_ref, w):
    def tile(rows):
        a = a_ref[rows, :]
        act = []
        for j in range(n):
            gu = dot(a, w_gu_of(w, u + j))
            act.append((jax.nn.silu(gu[:, :128]) * gu[:, 128:]).astype(BF))
        act = jnp.concatenate(act, axis=1) if n > 1 else act[0]
        for half in range(2):
            columns = slice(256 * half, 256 * half + 256)
            acc_ref[rows, columns] += dot(act, w_d_of(w, u, n, half))

    over(TILE, tile)


def backward_group(u, n, first, refs, sent):
    a_ref, a_t, dy_ref, dy_t, da_ref, w, w_t, w_dt, dgu_ref, act_ref = refs
    for j in range(n):
        if not first:
            w_t[256 * j : 256 * j + 256, :] = w_gu_of(w, u + j).T
    for half in range(2):
        w_dt[256 * half : 256 * half + 256, : 128 * n] = w_d_of(w, u, n, half).T

    def tile(rows):
        a = a_ref[rows, :]
        dact = dot(dy_ref[rows, :], w_dt[:, : 128 * n]).astype(BF).astype(F32)
        for j in range(n):
            gu = dot(a, w_gu_of(w, u + j))
            gate, up = gu[:, :128], gu[:, 128:]
            sig = jax.nn.sigmoid(gate)
            silu = gate * sig
            mine = dact[:, 128 * j : 128 * j + 128]
            act_ref[rows, 128 * j : 128 * j + 128] = (silu * up).astype(BF)
            dgu_ref[rows, 256 * j : 256 * j + 128] = (mine * up * (sig + silu * (1 - sig))).astype(BF)
            dgu_ref[rows, 256 * j + 128 : 256 * j + 256] = (mine * silu).astype(BF)
        if not first:
            da_ref[rows, :] += dot(dgu_ref[rows, : 256 * n], w_t[: 256 * n, :])

    over(TILE, tile)
    for j in range(n):
        sent(u + j)
        by_gu = dot(a_t[...], dgu_ref[:, 256 * j : 256 * j + 256]).astype(BF)
        w[u + j, :, :, :, :64, :] = by_gu.reshape(2, 2, 2, 64, 256)
    by_d = dot(dy_t[...], act_ref[:, : 128 * n])
    for j in range(n):
        for h in range(2):
            piece = by_d[256 * h : 256 * h + 256, 128 * j : 128 * j + 128].T.astype(BF)
            w[u + j, :, :, :, 64 + 16 * h : 80 + 16 * h, :] = piece.reshape(2, 2, 2, 16, 256)


def normed(h):
    wide, scale = rms(h)
    return (wide * scale).astype(BF)


def kernel(
    x_ref, dy_in, own, g_ref, a_kept, a_t_kept, h_ref, a_ref, a_t, dy_ref, dy_t, acc_ref, w, w_t, w_dt, dgu_ref, act_ref, r1, r2, r3, gsend, grecv, ssend, srecv, sem
):
    at = place()
    z1, z0, c, partners = at[:4]
    halves = [pl.ds(0, UNITS), pl.ds(UNITS, UNITS)]
    bring = [pltpu.make_async_copy(own.at[us], w.at[us, z1, z0, c], sem.at[i]) for i, us in enumerate(halves)]
    bring += [pltpu.make_async_copy(x_ref, h_ref, sem.at[2]), pltpu.make_async_copy(dy_in, dy_ref, sem.at[3])]
    for copy in bring:
        copy.start()
    bring[0].wait()
    bring[1].wait()
    greet(at)
    gather = functools.partial(gather_tick, w=w, send=gsend, recv=grecv, at=at)
    gather_first(gather, w, gsend, grecv, at)
    bring[2].wait()
    bring[3].wait()

    def enter(rows):
        a = normed(h_ref[rows, :])
        a_ref[rows, :] = a
        a_t[:, rows] = a.T
        dy_t[:, rows] = dy_ref[rows, :].T
        acc_ref[rows, :] = jnp.zeros((ROWS, D), F32)

    over(ROWS, enter)
    keep = [pltpu.make_async_copy(a_ref, a_kept, sem.at[0]), pltpu.make_async_copy(a_t, a_t_kept, sem.at[1])]
    for copy in keep:
        copy.start()

    def fetched(i, u, n):
        gather(i)
        for j in range(n):
            gather_ready(u + j, w, gsend, grecv, at)

    def forward(s, n):
        fetched(s + 4, 2 * s, n)
        forward_group(2 * s, n, a_ref, acc_ref, w)

    groups(forward)
    for copy in keep:
        copy.wait()

    def between(rows):
        h = h_ref[rows, :] + acc_ref[rows, :].astype(BF)
        h_ref[rows, :] = h
        a = normed(h)
        a_ref[rows, :] = a
        a_t[:, rows] = a.T
        acc_ref[rows, :] = jnp.zeros((ROWS, D), F32)

    over(ROWS, between)

    bufs = (w, r1, r2, r3)
    refs = (a_ref, a_t, dy_ref, dy_t, acc_ref, w, w_t, w_dt, dgu_ref, act_ref)

    def sent(u):
        gather_sent(u, w, gsend, grecv, at)

    def advance(stage, u, n):
        scatter_advance(stage, u, n, bufs, g_ref, ssend, srecv, at)

    def set_out(u, n):
        scatter_copy(0, u, n, bufs, ssend, srecv, at).start()

    end = UNITS - 1

    def layer1(s, n):
        u = UNITS + 2 * s
        fetched(s + GROUPS + 4, u, n)
        backward_group(u, n, False, refs, sent)
        for stage in range(3):
            back = u - 2 - 2 * stage

            @pl.when(back >= UNITS)
            def _(stage=stage, back=back):
                advance(stage, back, 2)

        set_out(u, n)

    groups(layer1)
    again = [pltpu.make_async_copy(a_kept, a_ref, sem.at[0]), pltpu.make_async_copy(a_t_kept, a_t, sem.at[1])]
    for copy in again:
        copy.start()

    def leave(rows):
        wide, scale = rms(h_ref[rows, :])
        da = acc_ref[rows, :].astype(BF).astype(F32)
        along = jnp.sum(da * wide, -1, keepdims=True) * (scale * scale * scale * (1.0 / D))
        dh = dy_ref[rows, :] + (da * scale - wide * along).astype(BF)
        dy_ref[rows, :] = dh
        dy_t[:, rows] = dh.T

    over(ROWS, leave)
    for copy in again:
        copy.wait()

    def layer0(s, n):
        u = 2 * s
        backward_group(u, n, True, refs, sent)
        for stage in range(3):
            back = u - 2 - 2 * stage

            @pl.when(back >= 0)
            def _(stage=stage, back=back):
                advance(stage, back, 2)

            @pl.when(back == -2)
            def _(stage=stage):
                advance(stage, BOTH - 1, 1)

            if stage:

                @pl.when(back < -2)
                def _(stage=stage, back=back):
                    advance(stage, back + BOTH + 1, 2)

        set_out(u, n)

    groups(layer0)
    for stage, u, n in ((0, end, 1), (1, end - 2, 2), (2, end - 4, 2), (1, end, 1), (2, end - 2, 2), (2, end, 1)):
        advance(stage, u, n)
    for stage in range(3):
        for base in (UNITS, 0):

            def one(s, carry, stage=stage, base=base):
                scatter_copy(stage, base + 2 * s, 2, bufs, ssend, srecv, at).wait_send()
                return carry

            lax.fori_loop(0, GROUPS - 1, one, 0)
            scatter_copy(stage, base + end, 1, bufs, ssend, srecv, at).wait_send()


def vmem(*shape):
    return pltpu.VMEM(shape, BF)


IN_VMEM = pl.BlockSpec(memory_space=pltpu.VMEM)
ANYWHERE = pl.BlockSpec(memory_space=pl.ANY)
DMA = pltpu.SemaphoreType.DMA


def gradients_of(x, dy, own):
    return pl.pallas_call(
        kernel,
        name="both_layers",
        out_shape=[jax.ShapeDtypeStruct(dims, BF) for dims in ((BOTH, 96, 256), (T, D), (D, T))],
        in_specs=[ANYWHERE] * 3,
        out_specs=[IN_VMEM, ANYWHERE, ANYWHERE],
        scratch_shapes=[
            vmem(T, D),
            vmem(T, D),
            vmem(D, T),
            vmem(T, D),
            vmem(D, T),
            pltpu.VMEM((T, D), F32),
            vmem(BOTH, 2, 2, 2, 96, 256),
            vmem(512, D),
            vmem(D, 256),
            vmem(T, 512),
            vmem(T, 256),
            vmem(BOTH, 2, 2, 96, 256),
            vmem(BOTH, 2, 96, 256),
            vmem(BOTH, 96, 256),
            *[DMA((4, BOTH))] * 2,
            *[DMA((3, BOTH))] * 2,
            DMA((4,)),
        ],
        compiler_params=pltpu.CompilerParams(collective_id=0, has_side_effects=True, vmem_limit_bytes=VMEM_LIMIT),
        cost_estimate=pl.CostEstimate(flops=34 * T * D * FF, bytes_accessed=20_000_000, transcendentals=0),
    )(x, dy, own)[0]


def to_units(w_gate, w_up, w_down):
    layers = w_gate.shape[0]
    wide = [w.reshape(layers, 64, 8, UNITS, 16).transpose(0, 3, 1, 2, 4).reshape(layers, UNITS, 64, 128) for w in (w_gate, w_up)]
    down = w_down.reshape(layers, UNITS, 16, 2, 256).transpose(0, 1, 3, 2, 4).reshape(layers, UNITS, 32, 256)
    return jnp.concatenate([jnp.concatenate(wide, -1), down], 2)


def from_units(g):
    layers = g.shape[0]
    wide = [
        g[:, :, :64, at : at + 128].reshape(layers, UNITS, 64, 8, 16).transpose(0, 2, 3, 1, 4).reshape(layers, 64, FF) for at in (0, 128)
    ]
    down = g[:, :, 64:].reshape(layers, UNITS, 2, 16, 256).transpose(0, 1, 3, 2, 4).reshape(layers, 208, D)
    return *wide, down


def adamw(w, m, v, g):
    m = 0.9 * m + 0.1 * g
    v = 0.95 * v + 0.05 * g * g
    step = m * lax.rsqrt(v + 1e-8) + 0.1 * w
    return (w - 0.02 * step).astype(BF), m, v


def solution(mesh):
    def step(x, dy, *arrays):
        weights, m, v = (arrays[i : i + 3] for i in (0, 3, 6))
        own = to_units(*weights)
        g = gradients_of(x[0], dy[0], own.reshape(BOTH, 96, 256))
        gradients = from_units(g.reshape(own.shape))
        new = [adamw(w.astype(F32), m, v, g.astype(F32)) for w, m, v, g in zip(weights, m, v, gradients, strict=True)]
        return tuple(one[which] for which in range(3) for one in new)

    states, cut = P(("rep", "dp"), None, None), P(None, "dp", None)
    return jax.shard_map(
        step,
        mesh=mesh,
        in_specs=(states, states) + (cut,) * 9,
        out_specs=(P("rep", "dp", None),) * 9,
        check_vma=False,
    )
```

```python
import functools

import jax
import jax.numpy as jnp
from jax import lax
from jax.experimental import pallas as pl
from jax.experimental.pallas import tpu as pltpu
from jax.sharding import PartitionSpec as P

T, D, FF = 4096, 512, 1664
UNITS = 13
GROUPS = 7
LAGS = (1, 2, 4)
TILE = 2048
ROWS = 512
PAIRS = UNITS
VMEM_LIMIT = 67_043_328
BF, F32 = jnp.bfloat16, jnp.float32
BOTH = 2 * UNITS


def dot(a, b):
    return lax.dot_general(a, b, (((1,), (0,)), ((), ())), preferred_element_type=F32)


def dot_nt(a, b):
    return lax.dot_general(a, b, (((1,), (1,)), ((), ())), preferred_element_type=F32)


def rms(h):
    wide = h.astype(F32)
    return wide, lax.rsqrt(jnp.mean(wide * wide, -1, keepdims=True) + 1e-6)


def place():
    me, rep = lax.axis_index("dp"), lax.axis_index("rep")
    z1, z0, c = lax.div(me, 4), lax.rem(lax.div(me, 2), 2), lax.rem(me, 2)
    x, y = lax.div(rep, 2), lax.rem(rep, 2)
    return z1, z0, c, (me + 1 - 2 * c, me + 2 - 4 * z0, me + 4 - 8 * z1), (x, y), (rep + 2 - 4 * x, rep + 1 - 2 * y)


def greet(at):
    barrier = pltpu.get_barrier_semaphore()
    for axis, partners in (("dp", at[3]), ("rep", at[5])):
        for p in partners:
            pl.semaphore_signal(barrier, inc=1, device_id={axis: p}, device_id_type=pl.DeviceIdType.MESH)
    pl.semaphore_wait(barrier, 5)


def turn(i, of):
    return of[0] + lax.rem(i, 2) * (of[1] - of[0])


def mine_of(i, at):
    return 2 * i + turn(i, at[4])


def gather_copy(stage, u, w, send, recv, at):
    z1, z0, c, partners, _, sides = at
    ref = (w.at[u, z1, z0, c], w.at[u, :, z0, c], w.at[u, :, :, c], w.at[u, :, :, c])[stage]
    to = ({"dp": partners[2]}, {"dp": partners[1]}, {"rep": turn(lax.div(u, 2), sides)}, {"dp": partners[0]})[stage]
    return pltpu.make_async_remote_copy(
        src_ref=ref,
        dst_ref=ref,
        send_sem=send.at[stage, u],
        recv_sem=recv.at[stage, u],
        device_id=to,
        device_id_type=pl.DeviceIdType.MESH,
    )


def gather_tick(i, w, send, recv, at):
    def copy(stage, u):
        return gather_copy(stage, u, w, send, recv, at)

    @pl.when(i < PAIRS)
    def _():
        copy(0, mine_of(i, at)).start()

    @pl.when((i >= 2) & (i < PAIRS + 1))
    def _():
        u = mine_of(i - 1, at)
        copy(0, u).wait_recv()
        copy(1, u).start()

    @pl.when((i >= 3) & (i < PAIRS + 2))
    def _():
        u = mine_of(i - 2, at)
        copy(1, u).wait_recv()
        copy(2, u).start()
        copy(3, u).start()

    @pl.when((i >= 4) & (i < PAIRS + 3))
    def _():
        u = 4 * (i - 3) + 1 - mine_of(i - 3, at)
        copy(2, u).wait_recv()
        copy(3, u).start()


def gather_first(tick, w, send, recv, at, meanwhile):
    for stage in range(3):
        for u in range(2):
            if stage:
                gather_copy(stage - 1, u, w, send, recv, at).wait_recv()
            gather_copy(stage + stage // 2, u, w, send, recv, at).start()
        tick(stage + 1)
        meanwhile(stage)


def gather_ready(u, w, send, recv, at):
    gather_copy(3, u, w, send, recv, at).wait_recv()


def gather_sent(u, w, send, recv, at):
    i = lax.div(u, 2)
    mine = u == mine_of(i, at)
    for stage, sent in ((0, mine | (i == 0)), (1, mine | (i == 0)), (2, mine & (i > 0))):

        @pl.when(sent)
        def _(stage=stage):
            gather_copy(stage, u, w, send, recv, at).wait_send()

    gather_copy(3, u, w, send, recv, at).wait_send()


def scatter_copy(stage, u, n, bufs, send, recv, at):
    z1, z0, c, partners = at[:4]
    own, r1, r2, r3 = bufs
    us = pl.ds(u, n)
    src = (own.at[us, :, :, 1 - c], r1.at[us, :, 1 - z0], r2.at[us, 1 - z1])[stage]
    dst = (r1, r2, r3)[stage].at[us]
    return pltpu.make_async_remote_copy(
        src_ref=src,
        dst_ref=dst,
        send_sem=send.at[stage, u],
        recv_sem=recv.at[stage, u],
        device_id={"dp": partners[stage]},
        device_id_type=pl.DeviceIdType.MESH,
    )


def scatter_advance(stage, u, n, bufs, g_ref, send, recv, at):
    z1, z0, c, partners = at[:4]
    own, r1, r2, r3 = bufs
    scatter_copy(stage, u, n, bufs, send, recv, at).wait_recv()
    for v in range(n):
        v = u + v
        if stage == 0:
            r1[v] = (r1[v].astype(F32) + own[v, :, :, c].astype(F32)).astype(BF)
        elif stage == 1:
            r2[v] = (r2[v].astype(F32) + r1[v, :, z0].astype(F32)).astype(BF)
        else:
            g_ref[v] = (r3[v].astype(F32) + r2[v, z1].astype(F32)).astype(BF)
    if stage < 2:
        scatter_copy(stage + 1, u, n, bufs, send, recv, at).start()


def over(tile, body):
    def one(t, carry):
        body(pl.ds(pl.multiple_of(t * tile, tile), tile))
        return carry

    lax.fori_loop(0, T // tile, one, 0)


def groups(body):
    def one(s, carry):
        body(s, 2)
        return carry

    lax.fori_loop(0, GROUPS - 1, one, 0)
    body(GROUPS - 1, 1)


def w_gu_of(w, u):
    return w[u, :, :, :, :64, :].reshape(D, 256)


def w_d_of(w, u, n, half):
    return w[pl.ds(u, n), :, :, :, 64 + 16 * half : 80 + 16 * half, :].reshape(n * 128, 256)


def forward_group(u, n, a_ref, acc_ref, w, halfway):
    def step(t, carry):
        pl.when(t == T // TILE // 2)(halfway)
        rows = pl.ds(pl.multiple_of(t * TILE, TILE), TILE)
        a = a_ref[rows, :]
        act = []
        for j in range(n):
            gu = dot(a, w_gu_of(w, u + j))
            act.append((jax.nn.silu(gu[:, :128]) * gu[:, 128:]).astype(BF))
        act = jnp.concatenate(act, axis=1) if n > 1 else act[0]
        for half in range(2):
            columns = slice(256 * half, 256 * half + 256)
            acc_ref[rows, columns] += dot(act, w_d_of(w, u, n, half))
        return carry

    lax.fori_loop(0, T // TILE, step, 0)


def backward_group(u, n, first, refs, sent):
    a_ref, a_t, dy_ref, dy_t, da_ref, w, w_t, w_dt, dgu_ref, act_ref = refs
    for j in range(n):
        if not first:
            w_t[256 * j : 256 * j + 256, :] = w_gu_of(w, u + j).T
    for half in range(2):
        w_dt[256 * half : 256 * half + 256, : 128 * n] = w_d_of(w, u, n, half).T

    def tile(rows):
        a = a_ref[rows, :]
        dact = dot(dy_ref[rows, :], w_dt[:, : 128 * n]).astype(BF).astype(F32)
        for j in range(n):
            gu = dot(a, w_gu_of(w, u + j))
            gate, up = gu[:, :128], gu[:, 128:]
            sig = jax.nn.sigmoid(gate)
            silu = gate * sig
            mine = dact[:, 128 * j : 128 * j + 128]
            act_ref[rows, 128 * j : 128 * j + 128] = (silu * up).astype(BF)
            dgu_ref[rows, 256 * j : 256 * j + 128] = (mine * up * (sig + silu * (1 - sig))).astype(BF)
            dgu_ref[rows, 256 * j + 128 : 256 * j + 256] = (mine * silu).astype(BF)
        if not first:
            da_ref[rows, :] += dot(dgu_ref[rows, : 256 * n], w_t[: 256 * n, :])

    over(TILE, tile)
    for j in range(n):
        sent(u + j)
        by_gu = dot(a_t[...], dgu_ref[:, 256 * j : 256 * j + 256]).astype(BF)
        w[u + j, :, :, :, :64, :] = by_gu.reshape(2, 2, 2, 64, 256)
    by_d = dot(dy_t[...], act_ref[:, : 128 * n])
    for j in range(n):
        for h in range(2):
            piece = by_d[256 * h : 256 * h + 256, 128 * j : 128 * j + 128].T.astype(BF)
            w[u + j, :, :, :, 64 + 16 * h : 80 + 16 * h, :] = piece.reshape(2, 2, 2, 16, 256)


def normed(h):
    wide, scale = rms(h)
    return (wide * scale).astype(BF)


def kernel(
    x_ref, dy_in, own, g_ref, a_kept, a_t_kept, h_ref, a_ref, a_t, dy_ref, dy_t, acc_ref, w, w_t, w_dt, dgu_ref, act_ref, r1, r2, r3, gsend, grecv, ssend, srecv, sem
):
    at = place()
    z1, z0, c, partners = at[:4]
    halves = [pl.ds(0, UNITS), pl.ds(UNITS, UNITS)]
    bring = [pltpu.make_async_copy(own.at[us], w.at[us, z1, z0, c], sem.at[i]) for i, us in enumerate(halves)]
    bring += [pltpu.make_async_copy(x_ref, h_ref, sem.at[2]), pltpu.make_async_copy(dy_in, dy_ref, sem.at[3])]
    for copy in bring:
        copy.start()
    bring[0].wait()
    bring[1].wait()
    greet(at)
    gather = functools.partial(gather_tick, w=w, send=gsend, recv=grecv, at=at)

    def enter(t, carry):
        rows = pl.ds(pl.multiple_of(t * ROWS, ROWS), ROWS)
        a = normed(h_ref[rows, :])
        a_ref[rows, :] = a
        a_t[:, rows] = a.T
        dy_t[:, rows] = dy_ref[rows, :].T
        acc_ref[rows, :] = jnp.zeros((ROWS, D), F32)
        return carry

    def meanwhile(stage):
        if stage == 0:
            bring[2].wait()
            bring[3].wait()
        if stage < 2:
            half = T // ROWS // 2
            lax.fori_loop(half * stage, half * stage + half, enter, 0)

    gather_first(gather, w, gsend, grecv, at, meanwhile)
    keep = [pltpu.make_async_copy(a_ref, a_kept, sem.at[0]), pltpu.make_async_copy(a_t, a_t_kept, sem.at[1])]
    for copy in keep:
        copy.start()

    def fetched(u, n):
        for j in range(n):
            gather_ready(u + j, w, gsend, grecv, at)

    def forward(s, n):
        fetched(2 * s, n)
        forward_group(2 * s, n, a_ref, acc_ref, w, lambda: gather(s + 4))

    groups(forward)
    for copy in keep:
        copy.wait()

    def between(rows):
        h = h_ref[rows, :] + acc_ref[rows, :].astype(BF)
        h_ref[rows, :] = h
        a = normed(h)
        a_ref[rows, :] = a
        a_t[:, rows] = a.T
        acc_ref[rows, :] = jnp.zeros((ROWS, D), F32)

    over(ROWS, between)

    bufs = (w, r1, r2, r3)
    refs = (a_ref, a_t, dy_ref, dy_t, acc_ref, w, w_t, w_dt, dgu_ref, act_ref)

    def sent(u):
        gather_sent(u, w, gsend, grecv, at)

    def advance(stage, u, n):
        scatter_advance(stage, u, n, bufs, g_ref, ssend, srecv, at)

    def set_out(u, n):
        scatter_copy(0, u, n, bufs, ssend, srecv, at).start()

    end = UNITS - 1

    def layer1(s, n):
        u = UNITS + 2 * s
        gather(s + GROUPS + 4)
        fetched(u, n)
        backward_group(u, n, False, refs, sent)
        for stage in range(3):
            back = u - 2 * LAGS[stage]

            @pl.when(back >= UNITS)
            def _(stage=stage, back=back):
                advance(stage, back, 2)

        set_out(u, n)

    groups(layer1)
    again = [pltpu.make_async_copy(a_kept, a_ref, sem.at[0]), pltpu.make_async_copy(a_t_kept, a_t, sem.at[1])]
    for copy in again:
        copy.start()

    def leave(rows):
        wide, scale = rms(h_ref[rows, :])
        da = acc_ref[rows, :].astype(BF).astype(F32)
        along = jnp.sum(da * wide, -1, keepdims=True) * (scale * scale * scale * (1.0 / D))
        dh = dy_ref[rows, :] + (da * scale - wide * along).astype(BF)
        dy_ref[rows, :] = dh
        dy_t[:, rows] = dh.T

    over(ROWS, leave)
    for copy in again:
        copy.wait()

    def layer0(s, n):
        u = 2 * s
        backward_group(u, n, True, refs, sent)
        for stage in range(3):
            back = u - 2 * LAGS[stage]

            @pl.when(back >= 0)
            def _(stage=stage, back=back):
                advance(stage, back, 2)

            @pl.when(back == -2)
            def _(stage=stage):
                advance(stage, BOTH - 1, 1)

            if stage:

                @pl.when(back < -2)
                def _(stage=stage, back=back):
                    advance(stage, back + BOTH + 1, 2)

        set_out(u, n)

    groups(layer0)
    for stage, back in ((0, 0), (1, 2), (2, 6), (2, 4), (1, 0), (2, 2), (2, 0)):
        advance(stage, end - back, 2 if back else 1)
    for stage in range(3):
        for base in (UNITS, 0):

            def one(s, carry, stage=stage, base=base):
                scatter_copy(stage, base + 2 * s, 2, bufs, ssend, srecv, at).wait_send()
                return carry

            lax.fori_loop(0, GROUPS - 1, one, 0)
            scatter_copy(stage, base + end, 1, bufs, ssend, srecv, at).wait_send()


def vmem(*shape):
    return pltpu.VMEM(shape, BF)


IN_VMEM = pl.BlockSpec(memory_space=pltpu.VMEM)
ANYWHERE = pl.BlockSpec(memory_space=pl.ANY)
DMA = pltpu.SemaphoreType.DMA


def gradients_of(x, dy, own):
    return pl.pallas_call(
        kernel,
        name="both_layers",
        out_shape=[jax.ShapeDtypeStruct(dims, BF) for dims in ((BOTH, 96, 256), (T, D), (D, T))],
        in_specs=[ANYWHERE] * 3,
        out_specs=[IN_VMEM, ANYWHERE, ANYWHERE],
        scratch_shapes=[
            vmem(T, D),
            vmem(T, D),
            vmem(D, T),
            vmem(T, D),
            vmem(D, T),
            pltpu.VMEM((T, D), F32),
            vmem(BOTH, 2, 2, 2, 96, 256),
            vmem(512, D),
            vmem(D, 256),
            vmem(T, 512),
            vmem(T, 256),
            vmem(BOTH, 2, 2, 96, 256),
            vmem(BOTH, 2, 96, 256),
            vmem(BOTH, 96, 256),
            *[DMA((4, BOTH))] * 2,
            *[DMA((3, BOTH))] * 2,
            DMA((4,)),
        ],
        compiler_params=pltpu.CompilerParams(collective_id=0, has_side_effects=True, vmem_limit_bytes=VMEM_LIMIT),
        cost_estimate=pl.CostEstimate(flops=34 * T * D * FF, bytes_accessed=20_000_000, transcendentals=0),
    )(x, dy, own)[0]


def to_units(w_gate, w_up, w_down):
    layers = w_gate.shape[0]
    wide = [w.reshape(layers, 64, 8, UNITS, 16).transpose(0, 3, 1, 2, 4).reshape(layers, UNITS, 64, 128) for w in (w_gate, w_up)]
    down = w_down.reshape(layers, UNITS, 16, 2, 256).transpose(0, 1, 3, 2, 4).reshape(layers, UNITS, 32, 256)
    return jnp.concatenate([jnp.concatenate(wide, -1), down], 2)


def from_units(g):
    layers = g.shape[0]
    wide = [
        g[:, :, :64, at : at + 128].reshape(layers, UNITS, 64, 8, 16).transpose(0, 2, 3, 1, 4).reshape(layers, 64, FF) for at in (0, 128)
    ]
    down = g[:, :, 64:].reshape(layers, UNITS, 2, 16, 256).transpose(0, 1, 3, 2, 4).reshape(layers, 208, D)
    return *wide, down


def adamw(w, m, v, g):
    m = 0.9 * m + 0.1 * g
    v = 0.95 * v + 0.05 * g * g
    step = m * lax.rsqrt(v + 1e-8) + 0.1 * w
    return (w - 0.02 * step).astype(BF), m, v


def solution(mesh):
    def step(x, dy, *arrays):
        weights, m, v = (arrays[i : i + 3] for i in (0, 3, 6))
        own = to_units(*weights)
        g = gradients_of(x[0], dy[0], own.reshape(BOTH, 96, 256))
        gradients = from_units(g.reshape(own.shape))
        new = [adamw(w.astype(F32), m, v, g.astype(F32)) for w, m, v, g in zip(weights, m, v, gradients, strict=True)]
        return tuple(one[which] for which in range(3) for one in new)

    states, cut = P(("rep", "dp"), None, None), P(None, "dp", None)
    return jax.shard_map(
        step,
        mesh=mesh,
        in_specs=(states, states) + (cut,) * 9,
        out_specs=(P("rep", "dp", None),) * 9,
        check_vma=False,
    )
```
